32 devices in a mesh: grp: 2 (over y), mem: 16 (over z, x, core).
Axes of the slice: x: 2, y: 2, z: 4, core: 2. Of those that a mesh axis runs over, the one named last changes fastest.
Arguments:
- tokens: bfloat16 [4096, 1024], P(('grp', 'mem')), may hold values from -6 to 6
- cotangent: bfloat16 [4096, 1024], P(('grp', 'mem')), may hold values from -6 to 6
- path: int32 [32, 3], P(('grp', 'mem')), may hold values from 0 to 63, as said below
- coarse_weights: bfloat16 [4, 1024, 512], P(None, 'mem'), may hold values from -0.1875 to 0.1875
- middle_weights: bfloat16 [64, 1024, 256], P(None, 'mem'), may hold values from -0.1875 to 0.1875
- fine_weights: bfloat16 [64, 1024, 128], P('grp', 'mem'), may hold values from -0.1875 to 0.1875
Outputs:
- tokens_grad: bfloat16 [4096, 1024], P(('grp', 'mem'))
- coarse_grad: bfloat16 [4, 1024, 512], P(None, 'mem')
- middle_grad: bfloat16 [64, 1024, 256], P(None, 'mem')
- fine_grad: bfloat16 [64, 1024, 128], P('grp', 'mem')
The draws below stay inside these ranges and needn't reach their ends.
Inputs may be any that keep to these rules, and one draw needn't show every extreme that they name: Row d is the path of document d: column 0 its coarse block, column 1 its middle block, column 2 its fine block, with middle = fine * 1 and coarse = middle * 4 // 64. Some fine blocks are chosen by many documents.
All inputs are finite; a program needn't handle non-finite values.
Results may differ from the reference program's by a relative error of at most 0.005.
Values may be sent and summed in bfloat16 or wider, within the bound.
A program may use at most 64 MiB of HBM per device.

```python
from functools import partial
import jax
import jax.numpy as jnp
from jax import lax

D = 1024
HC = 256
HM = 128
HF = 64
COARSE = 4
MIDDLE = 64
TOK_DEV = 128
FINE = 64
DOCS = 32
TOKENS = 4096


def draw_path(key, part):
    first, second, third, fourth = jax.random.split(key, 4)
    fine_ids = jax.random.randint(first, (DOCS,), 0, FINE)
    popular = jax.random.randint(second, (8,), 0, FINE)
    chooser = jax.random.randint(third, (DOCS,), 0, 32)
    fine_ids = jnp.where(chooser < 8, popular[chooser % 8], fine_ids)
    places = jax.random.permutation(fourth, DOCS)
    fine_ids = fine_ids.at[places[0]].set(0).at[places[1]].set(FINE - 1)
    middle_ids = fine_ids * MIDDLE // FINE
    coarse_ids = middle_ids * COARSE // MIDDLE
    return jnp.stack([coarse_ids, middle_ids, fine_ids], axis=1).astype(jnp.int32)


def steps_of(stream_key, dims, shards, smallest, top_value):
    def one(dim, shards_of):
        draws = jax.random.uniform(jax.random.fold_in(jax.random.fold_in(stream_key, 6), dim), (shards_of,), jnp.float32, smallest / len(shards), top_value / len(shards))
        return jnp.repeat(jnp.exp(draws), dims[dim] // shards_of).reshape((-1,) + (1,) * (len(dims) - dim - 1))

    loudness = one(*shards[0])
    for cut in shards[1:]:
        loudness = loudness * one(*cut)
    return loudness


def bell_draw(stream_key, dims, width, most, cuts=(), kind=jnp.bfloat16):
    entries = width * jax.random.normal(stream_key, dims, jnp.float32)
    if cuts:
        entries = entries * steps_of(stream_key, dims, cuts, -0.22, 0.18)
    return jnp.clip(entries, -most, most).astype(kind)


def setup_inputs(seed: int = 0) -> dict:
    streams_of = jax.random.split(jax.random.key(seed), 7)
    tokens = bell_draw(streams_of[0], (TOKENS, D), 1.0, 6.0, ((0, 32),))
    cotangent = bell_draw(streams_of[1], (TOKENS, D), 1.0, 6.0, ((0, 32),))
    path = draw_path(jax.random.fold_in(streams_of[6], 71), 0)
    coarse_weights = bell_draw(streams_of[3], (COARSE, D, 2 * HC), D ** -0.5, 0.1875, ((1, 16),))
    middle_weights = bell_draw(streams_of[4], (MIDDLE, D, 2 * HM), D ** -0.5, 0.1875, ((1, 16),))
    fine_weights = bell_draw(streams_of[5], (FINE, D, 2 * HF), D ** -0.5, 0.1875, ((0, 2), (1, 16)))
    return dict(tokens=tokens, cotangent=cotangent, path=path, coarse_weights=coarse_weights, middle_weights=middle_weights, fine_weights=fine_weights)


def contract_rows(left, right):
    return lax.dot_general(left, right, (((0,), (0,)), ((), ())), preferred_element_type=jnp.float32)

def level_terms(inputs, upstream, weights):
    hidden_width = weights.shape[1] // 2
    up_half = weights[:, :hidden_width]
    down_half = weights[:, hidden_width:]
    before = jnp.dot(inputs, up_half, preferred_element_type=jnp.float32)
    hidden, pullback = jax.vjp(partial(jax.nn.gelu, approximate=True), before)
    hidden_low = hidden.astype(jnp.bfloat16)
    hidden_grad = jnp.dot(upstream, down_half, preferred_element_type=jnp.float32)
    before_grad = pullback(hidden_grad)[0].astype(jnp.bfloat16)
    up_grad = contract_rows(inputs, before_grad)
    down_grad = contract_rows(upstream, hidden_low)
    input_part = lax.dot_general(before_grad, up_half, (((1,), (1,)), ((), ())), preferred_element_type=jnp.float32)
    return (jnp.concatenate([up_grad, down_grad], axis=1), input_part)

def reference(tokens, cotangent, path, coarse_weights, middle_weights, fine_weights):
    documents = path.shape[0]
    token_blocks = tokens.reshape(documents, TOK_DEV, D)
    upstream_blocks = cotangent.reshape(documents, TOK_DEV, D)
    start = (jnp.zeros(coarse_weights.shape, jnp.float32), jnp.zeros(middle_weights.shape, jnp.float32), jnp.zeros(fine_weights.shape, jnp.float32))

    def advance(carry, item):
        inputs, upstream, route = item
        coarse_sum, middle_sum, fine_sum = carry
        coarse_term, coarse_back = level_terms(inputs, upstream, coarse_weights[route[0]])
        middle_term, middle_back = level_terms(inputs, upstream, middle_weights[route[1]])
        fine_term, fine_back = level_terms(inputs, upstream, fine_weights[route[2]])
        coarse_sum = coarse_sum.at[route[0]].add(coarse_term)
        middle_sum = middle_sum.at[route[1]].add(middle_term)
        fine_sum = fine_sum.at[route[2]].add(fine_term)
        summed = (coarse_back + middle_back + fine_back).astype(jnp.bfloat16)
        return ((coarse_sum, middle_sum, fine_sum), summed)
    totals, input_grads = lax.scan(advance, start, (token_blocks, upstream_blocks, path))
    return (input_grads.reshape(documents * TOK_DEV, D), totals[0].astype(jnp.bfloat16), totals[1].astype(jnp.bfloat16), totals[2].astype(jnp.bfloat16))
```

```python
import functools
import math

import jax
import jax.numpy as jnp
from jax import lax
from jax.experimental import pallas as pl
from jax.experimental.pallas import tpu as pltpu
from jax.sharding import PartitionSpec as P

MESH = pl.DeviceIdType.MESH
LANES = 128
F32 = jnp.float32
BF16 = jnp.bfloat16


def path_kernel(groups, members, row_ref, all_ref, send_sem, recv_sem):
    group = lax.axis_index("grp")
    member = lax.axis_index("mem")
    count = groups * members
    me = group * members + member
    barrier = pltpu.get_barrier_semaphore()

    def place(step):
        other = lax.rem(me + step, count)
        return other, (other // members, lax.rem(other, members))

    def greet(step, carry):
        _, where = place(step)
        pl.semaphore_signal(barrier, inc=1, device_id=where, device_id_type=MESH)
        return carry

    lax.fori_loop(1, count, greet, 0)
    pl.semaphore_wait(barrier, count - 1)

    def copy(step):
        other, where = place(step)
        return other, where

    def send(step, carry):
        other, where = place(step)
        pltpu.make_async_remote_copy(
            src_ref=row_ref.at[0],
            dst_ref=all_ref.at[me],
            send_sem=send_sem.at[other],
            recv_sem=recv_sem.at[me],
            device_id=where,
            device_id_type=MESH,
        ).start()
        return carry

    lax.fori_loop(1, count, send, 0)
    all_ref[me] = row_ref[0]

    def finish(step, carry):
        other, where = place(step)
        done = pltpu.make_async_remote_copy(
            src_ref=row_ref.at[0],
            dst_ref=all_ref.at[other],
            send_sem=send_sem.at[other],
            recv_sem=recv_sem.at[other],
            device_id=where,
            device_id_type=MESH,
        )
        done.wait_send()
        done.wait_recv()
        return carry

    lax.fori_loop(1, count, finish, 0)


def gather_paths(path, groups, members):
    count = groups * members
    row = jnp.pad(path, ((0, 0), (0, LANES - path.shape[1])))[:, None, :]
    out = pl.pallas_call(
        functools.partial(path_kernel, groups, members),
        out_shape=jax.ShapeDtypeStruct((count, 1, LANES), jnp.int32),
        in_specs=[pl.BlockSpec(memory_space=pltpu.VMEM)],
        out_specs=pl.BlockSpec(memory_space=pltpu.VMEM),
        scratch_shapes=[
            pltpu.SemaphoreType.DMA((count,)),
            pltpu.SemaphoreType.DMA((count,)),
        ],
        compiler_params=pltpu.CompilerParams(collective_id=0, has_side_effects=True),
        name="path_gather",
    )(row)
    return out[:, 0, : path.shape[1]].reshape(-1)


def gelu_parts(before, hidden_grad):
    scale = math.sqrt(2.0 / math.pi)
    square = before * before
    tanh = jnp.tanh(scale * (before + 0.044715 * (square * before)))
    half = 0.5 * (1.0 + tanh)
    hidden = before * half
    slope = half + 0.5 * before * (1.0 - tanh * tanh) * (scale * (1.0 + 3 * 0.044715 * square))
    return hidden.astype(BF16), (hidden_grad * slope).astype(BF16)


def dot(left, right):
    return jnp.dot(left, right, preferred_element_type=F32)


def dot_transposed(left, right):
    return lax.dot_general(left, right, (((1,), (1,)), ((), ())), preferred_element_type=F32)


def level(weights, x, g, xt, gt):
    width = weights.shape[1]
    half = width // 2
    if half % LANES == 0:
        up = weights[:, :half]
        down = weights[:, half:]
        hidden, grad = gelu_parts(dot(x, up), dot(g, down))
        term = jnp.concatenate(
            [dot(xt, grad).astype(BF16), dot(gt, hidden).astype(BF16)], axis=1
        )
        return term, dot_transposed(grad, up)
    before = dot(x, weights)
    hidden_grad = pltpu.roll(dot(g, weights), half, 1)
    hidden, grad = gelu_parts(before, hidden_grad)
    first = lax.broadcasted_iota(jnp.int32, grad.shape, 1) < half
    grad = jnp.where(first, grad.astype(F32), 0.0).astype(BF16)
    hidden = jnp.where(first, hidden.astype(F32), 0.0)
    hidden = pltpu.roll(hidden, half, 1).astype(BF16)
    term = (dot(xt, grad) + dot(gt, hidden)).astype(BF16)
    return term, dot_transposed(grad, weights)


def main_kernel(
    groups,
    members,
    path,
    tokens,
    cotangent,
    coarse_w,
    middle_w,
    fine_w,
    tokens_grad,
    middle_parts,
    fine_parts,
    coarse_own,
    coarse_others,
    coarse_send,
    middle_send,
    fine_out,
    fine_in,
    fine_send,
    coarse_block,
    middle_block,
    fine_block,
    coarse_term,
    middle_term,
    fine_term,
    coarse_parts,
    coarse_half,
    xt,
    gt,
    total,
    mem_send,
    mem_recv,
    grp_send,
    grp_recv,
):
    group = lax.axis_index("grp")
    me = lax.axis_index("mem")
    owned = fine_w.shape[0]

    barrier = pltpu.get_barrier_semaphore()

    def greet_member(step, carry):
        pl.semaphore_signal(
            barrier,
            inc=1,
            device_id={"mem": lax.rem(me + step, members)},
            device_id_type=MESH,
        )
        return carry

    def greet_group(step, carry):
        pl.semaphore_signal(
            barrier,
            inc=1,
            device_id={"grp": lax.rem(group + step, groups)},
            device_id_type=MESH,
        )
        return carry

    lax.fori_loop(1, members, greet_member, 0)
    lax.fori_loop(1, groups, greet_group, 0)

    def route(document, column):
        return path[document * 3 + column]

    def pick_fine(index, carry):
        identity = route(index, 2)
        place = jnp.clip(identity - group * owned, 0, owned - 1)
        fine_out[index // members, lax.rem(index, members)] = fine_w[place]
        return carry

    lax.fori_loop(0, groups * members, pick_fine, 0)

    def pick_middle(p, carry):
        middle_send[p] = middle_w[route(group * members + p, 1)]
        return carry

    def pick_coarse(p, carry):
        coarse_send[p] = coarse_w[route(group * members + p, 0)]
        return carry

    lax.fori_loop(0, members, pick_middle, 0)

    pl.semaphore_wait(barrier, members - 1 + groups - 1)

    def member_copy(slot, source, target, out_slot, in_slot, p):
        return pltpu.make_async_remote_copy(
            src_ref=source.at[out_slot],
            dst_ref=target.at[in_slot],
            send_sem=mem_send.at[slot, p],
            recv_sem=mem_recv.at[slot, in_slot],
            device_id={"mem": p},
            device_id_type=MESH,
        )

    def spread(slot, source, target):
        def body(step, carry):
            p = lax.rem(me + step, members)
            member_copy(slot, source, target, p, me, p).start()
            return carry

        lax.fori_loop(1, members, body, 0)

    def arrive(slot, source, target):
        def body(step, carry):
            p = lax.rem(me + members - step, members)
            member_copy(slot, source, target, p, p, p).wait_recv()
            return carry

        lax.fori_loop(1, members, body, 0)

    def left(slot, source, target):
        def body(step, carry):
            p = lax.rem(me + step, members)
            member_copy(slot, source, target, p, p, p).wait_send()
            return carry

        lax.fori_loop(1, members, body, 0)

    def group_copy(slot, source, target, in_slot, other):
        return pltpu.make_async_remote_copy(
            src_ref=source,
            dst_ref=target.at[in_slot],
            send_sem=grp_send.at[slot, other],
            recv_sem=grp_recv.at[slot, in_slot],
            device_id={"grp": other},
            device_id_type=MESH,
        )

    def group_spread(slot, source_of, target):
        def body(step, carry):
            other = lax.rem(group + step, groups)
            group_copy(slot, source_of(other), target, group, other).start()
            return carry

        lax.fori_loop(1, groups, body, 0)

    def group_arrive(slot, source_of, target):
        def body(step, carry):
            other = lax.rem(group + step, groups)
            group_copy(slot, source_of(other), target, other, other).wait_recv()
            return carry

        lax.fori_loop(1, groups, body, 0)

    def group_left(slot, source_of, target):
        def body(step, carry):
            other = lax.rem(group + step, groups)
            group_copy(slot, source_of(other), target, other, other).wait_send()
            return carry

        lax.fori_loop(1, groups, body, 0)

    fine_source = lambda other: fine_out.at[other]
    group_spread(0, fine_source, fine_in)
    spread(0, middle_send, middle_block)
    middle_block[me] = middle_send[me]
    lax.fori_loop(0, members, pick_coarse, 0)
    coarse_block[me] = coarse_send[me]
    fine_in[group] = fine_out[group]
    group_arrive(0, fine_source, fine_in)

    def merge_fine(p, carry):
        owner = route(group * members + p, 2) // owned
        fine_send[p] = fine_in[owner, p]
        return carry

    lax.fori_loop(0, members, merge_fine, 0)
    spread(1, fine_send, fine_block)
    spread(2, coarse_send, coarse_block)
    fine_block[me] = fine_send[me]

    width = tokens.shape[1]
    for start in range(0, width, LANES):
        columns = slice(start, start + LANES)
        xt[columns, :] = tokens[:, columns].T
        gt[columns, :] = cotangent[:, columns].T

    def compute(block, term):
        weights = block[...].reshape(width, block.shape[2])
        value, part = level(weights, tokens[...], cotangent[...], xt[...], gt[...])
        term[...] = value.reshape(term.shape)
        return part

    middle_own = middle_parts.at[group]
    fine_own = fine_parts.at[group]

    arrive(0, middle_send, middle_block)
    total[...] = compute(middle_block, middle_term)
    spread(3, middle_term, middle_own)
    middle_parts[group, me] = middle_term[me]

    arrive(1, fine_send, fine_block)
    total[...] += compute(fine_block, fine_term)
    spread(4, fine_term, fine_own)
    fine_parts[group, me] = fine_term[me]

    arrive(2, coarse_send, coarse_block)
    part = compute(coarse_block, coarse_term)
    spread(5, coarse_term, coarse_parts)
    coarse_parts[me] = coarse_term[me]
    tokens_grad[...] = (total[...] + part).astype(BF16)

    arrive(3, middle_term, middle_own)
    middle_source = lambda other: middle_own
    group_spread(1, middle_source, middle_parts)
    arrive(4, fine_term, fine_own)
    fine_own_source = lambda other: fine_own
    group_spread(2, fine_own_source, fine_parts)

    left(0, middle_send, middle_block)
    left(1, fine_send, fine_block)
    left(2, coarse_send, coarse_block)
    group_left(0, fine_source, fine_in)
    left(3, middle_term, middle_own)
    left(4, fine_term, fine_own)

    coarse_own[...] = jnp.zeros_like(coarse_own)
    coarse_others[group] = jnp.zeros(coarse_others.shape[1:], BF16)
    arrive(5, coarse_term, coarse_parts)

    def add_coarse(p, carry):
        identity = route(group * members + p, 0)
        piece = coarse_parts[p].astype(F32)
        for k in range(coarse_own.shape[0]):
            coarse_own[k] += piece * jnp.where(identity == k, 1.0, 0.0)
        return carry

    lax.fori_loop(0, members, add_coarse, 0)
    coarse_half[...] = coarse_own[...].astype(BF16)
    coarse_source = lambda other: coarse_half
    group_spread(3, coarse_source, coarse_others)
    left(5, coarse_term, coarse_parts)
    group_arrive(1, middle_source, middle_parts)
    group_arrive(2, fine_own_source, fine_parts)
    group_arrive(3, coarse_source, coarse_others)
    group_left(1, middle_source, middle_parts)
    group_left(2, fine_own_source, fine_parts)
    group_left(3, coarse_source, coarse_others)


def exchange(paths, tokens, cotangent, coarse_w, middle_w, fine_w, groups, members):
    rows = coarse_w.shape[1]
    wide, medium, narrow = coarse_w.shape[2], middle_w.shape[2], fine_w.shape[2]
    token_count, width = tokens.shape

    def stack(size, kind=BF16):
        return pltpu.VMEM((members, rows, size), kind)

    vmem = pl.BlockSpec(memory_space=pltpu.VMEM)
    return pl.pallas_call(
        functools.partial(main_kernel, groups, members),
        out_shape=(
            jax.ShapeDtypeStruct(tokens.shape, BF16),
            jax.ShapeDtypeStruct((groups, members, rows, medium), BF16),
            jax.ShapeDtypeStruct((groups, members, rows, narrow), BF16),
            jax.ShapeDtypeStruct(coarse_w.shape, F32),
            jax.ShapeDtypeStruct((groups,) + coarse_w.shape, BF16),
        ),
        in_specs=[pl.BlockSpec(memory_space=pltpu.SMEM)] + [vmem] * 5,
        out_specs=(vmem,) * 5,
        scratch_shapes=[
            stack(wide),
            stack(medium),
            pltpu.VMEM((groups, members, rows, narrow), BF16),
            pltpu.VMEM((groups, members, rows, narrow), BF16),
            stack(narrow),
            stack(wide),
            stack(medium),
            stack(narrow),
            stack(wide),
            stack(medium),
            stack(narrow),
            stack(wide),
            pltpu.VMEM(coarse_w.shape, BF16),
            pltpu.VMEM((width, token_count), BF16),
            pltpu.VMEM((width, token_count), BF16),
            pltpu.VMEM((token_count, width), F32),
            pltpu.SemaphoreType.DMA((6, members)),
            pltpu.SemaphoreType.DMA((6, members)),
            pltpu.SemaphoreType.DMA((4, groups)),
            pltpu.SemaphoreType.DMA((4, groups)),
        ],
        compiler_params=pltpu.CompilerParams(
            collective_id=1, has_side_effects=True, vmem_limit_bytes=60 * 2**20
        ),
        name="exchange",
    )(paths, tokens, cotangent, coarse_w, middle_w, fine_w)


def collect_kernel(
    path,
    first_owned,
    middle_parts,
    fine_parts,
    coarse_own,
    coarse_others,
    coarse_grad,
    middle_grad,
    fine_grad,
    middle_sum,
    fine_sum,
):
    owned = fine_grad.shape[0]
    middle_sum[...] = jnp.zeros_like(middle_sum)
    fine_sum[...] = jnp.zeros_like(fine_sum)

    def add(document, carry):
        k = path[document * 3 + 1]
        middle_sum[k] += middle_parts[document].astype(F32)
        place = path[document * 3 + 2] - first_owned[0]

        @pl.when((place >= 0) & (place < owned))
        def _():
            fine_sum[place] += fine_parts[document].astype(F32)

        return carry

    lax.fori_loop(0, middle_parts.shape[0], add, 0)
    middle_grad[...] = middle_sum[...].astype(BF16)
    fine_grad[...] = fine_sum[...].astype(BF16)
    coarse = coarse_own[...]
    for other in range(coarse_others.shape[0]):
        coarse = coarse + coarse_others[other].astype(F32)
    coarse_grad[...] = coarse.astype(BF16)


def collect(paths, first_owned, middle_parts, fine_parts, coarse_own, coarse_others, shapes):
    vmem = pl.BlockSpec(memory_space=pltpu.VMEM)
    smem = pl.BlockSpec(memory_space=pltpu.SMEM)
    return pl.pallas_call(
        collect_kernel,
        out_shape=tuple(jax.ShapeDtypeStruct(shape, BF16) for shape in shapes),
        in_specs=[smem, smem] + [vmem] * 4,
        out_specs=(vmem,) * 3,
        scratch_shapes=[pltpu.VMEM(shapes[1], F32), pltpu.VMEM(shapes[2], F32)],
        compiler_params=pltpu.CompilerParams(vmem_limit_bytes=60 * 2**20),
        name="collect",
    )(paths, first_owned, middle_parts, fine_parts, coarse_own, coarse_others)


def on_device(tokens, cotangent, path, coarse_weights, middle_weights, fine_weights):
    members = lax.axis_size("mem")
    groups = lax.axis_size("grp")
    paths = gather_paths(path, groups, members)
    tokens_grad, middle_parts, fine_parts, coarse_own, coarse_others = exchange(
        paths, tokens, cotangent, coarse_weights, middle_weights, fine_weights, groups, members
    )
    first_owned = (lax.axis_index("grp") * fine_weights.shape[0]).astype(jnp.int32).reshape(1)
    flat = lambda parts: parts.reshape((groups * members,) + parts.shape[2:])
    grads = collect(
        paths,
        first_owned,
        flat(middle_parts),
        flat(fine_parts),
        coarse_own,
        coarse_others,
        (coarse_weights.shape, middle_weights.shape, fine_weights.shape),
    )
    return (tokens_grad,) + tuple(grads)


def solution(mesh):
    return jax.shard_map(
        on_device,
        mesh=mesh,
        in_specs=(
            P(("grp", "mem"), None),
            P(("grp", "mem"), None),
            P(("grp", "mem"), None),
            P(None, "mem", None),
            P(None, "mem", None),
            P("grp", "mem", None),
        ),
        out_specs=(
            P(("grp", "mem"), None),
            P(None, "mem", None),
            P(None, "mem", None),
            P("grp", "mem", None),
        ),
        check_vma=False,
    )
```

```python
import functools
import math

import jax
import jax.numpy as jnp
from jax import lax
from jax.experimental import pallas as pl
from jax.experimental.pallas import tpu as pltpu
from jax.sharding import PartitionSpec as P

MESH = pl.DeviceIdType.MESH
LANES = 128
F32 = jnp.float32
BF16 = jnp.bfloat16


def gelu_parts(before, hidden_grad):
    scale = math.sqrt(2.0 / math.pi)
    square = before * before
    tanh = jnp.tanh(scale * (before + 0.044715 * (square * before)))
    half = 0.5 * (1.0 + tanh)
    hidden = before * half
    slope = half + 0.5 * before * (1.0 - tanh * tanh) * (scale * (1.0 + 3 * 0.044715 * square))
    return hidden.astype(BF16), (hidden_grad * slope).astype(BF16)


def dot(left, right):
    return jnp.dot(left, right, preferred_element_type=F32)


def dot_transposed(left, right):
    return lax.dot_general(left, right, (((1,), (1,)), ((), ())), preferred_element_type=F32)


def level(weights, x, g, xt, gt):
    width = weights.shape[1]
    half = width // 2
    if half % LANES == 0:
        up = weights[:, :half]
        down = weights[:, half:]
        hidden, grad = gelu_parts(dot(x, up), dot(g, down))
        term = jnp.concatenate(
            [dot(xt, grad).astype(BF16), dot(gt, hidden).astype(BF16)], axis=1
        )
        return term, dot_transposed(grad, up)
    before = dot(x, weights)
    hidden_grad = pltpu.roll(dot(g, weights), half, 1)
    hidden, grad = gelu_parts(before, hidden_grad)
    first = lax.broadcasted_iota(jnp.int32, grad.shape, 1) < half
    grad = jnp.where(first, grad.astype(F32), 0.0).astype(BF16)
    hidden = jnp.where(first, hidden.astype(F32), 0.0)
    hidden = pltpu.roll(hidden, half, 1).astype(BF16)
    term = (dot(xt, grad) + dot(gt, hidden)).astype(BF16)
    return term, dot_transposed(grad, weights)


def plan(groups, members, blocks_width):
    inner = max(k for k in range(1, math.isqrt(members) + 1) if members % k == 0)
    team = math.gcd(groups, blocks_width // LANES)
    return members // inner, inner, team


def main_kernel(
    groups,
    members,
    path_row,
    tokens,
    cotangent,
    coarse_w,
    middle_w,
    fine_w,
    all_paths,
    tokens_grad,
    middle_parts,
    fine_parts,
    coarse_parts,
    path,
    middle_send,
    fine_out,
    fine_in,
    fine_send,
    coarse_line,
    coarse_send,
    coarse_block,
    middle_block,
    fine_block,
    coarse_term,
    middle_term,
    fine_term,
    coarse_terms_in,
    coarse_sums,
    coarse_sums_in,
    coarse_total,
    xt,
    gt,
    total,
    path_send,
    path_recv,
    mem_send,
    mem_recv,
    grp_send,
    grp_recv,
    line_send,
    line_recv,
    team_send,
    team_recv,
    local_sem,
):
    group = lax.axis_index("grp")
    me = lax.axis_index("mem")
    count = groups * members
    device = group * members + me
    owned = fine_w.shape[0]
    coarse_count, rows, wide = coarse_w.shape
    outer, inner, team = plan(groups, members, wide)
    size = team * inner
    columns = wide // team
    line = me // inner
    place = lax.rem(me, inner)
    slot = lax.rem(group, team)
    team_first = group - slot
    spot = slot * inner + place

    def loop(start, stop, body):
        def wrapped(step, carry):
            body(step)
            return carry

        lax.fori_loop(start, stop, wrapped, 0)

    def column_range(s):
        return pl.ds(pl.multiple_of(s * columns, LANES), columns)

    barrier = pltpu.get_barrier_semaphore()

    def anyone(step):
        other = lax.rem(device + step, count)
        return other, (other // members, lax.rem(other, members))

    def greet(step):
        _, where = anyone(step)
        pl.semaphore_signal(barrier, inc=1, device_id=where, device_id_type=MESH)

    loop(1, count, greet)
    own_columns = coarse_w.at[:, :, column_range(slot)]
    line_self = pltpu.make_async_copy(own_columns, coarse_line.at[line], local_sem.at[0])
    line_self.start()
    pl.semaphore_wait(barrier, count - 1)

    def path_copy(step, landing_own):
        other, where = anyone(step)
        return pltpu.make_async_remote_copy(
            src_ref=path_row,
            dst_ref=all_paths.at[device if landing_own else other],
            send_sem=path_send.at[other],
            recv_sem=path_recv.at[device if landing_own else other],
            device_id=where,
            device_id_type=MESH,
        )

    loop(1, count, lambda step: path_copy(step, True).start())
    all_paths[device] = path_row[...]

    def line_copy(index, source, target, step, landing_own):
        other = lax.rem(line + step, outer)
        landing = line if landing_own else other
        return pltpu.make_async_remote_copy(
            src_ref=source(other),
            dst_ref=target.at[landing],
            send_sem=line_send.at[index, other],
            recv_sem=line_recv.at[index, landing],
            device_id={"mem": other * inner + place},
            device_id_type=MESH,
        )

    first_stage = (0, lambda other: own_columns, coarse_line)
    loop(1, outer, lambda step: line_copy(*first_stage, step, True).start())

    width = tokens.shape[1]
    for start in range(0, width, LANES):
        part = slice(start, start + LANES)
        xt[part, :] = tokens[:, part].T
        gt[part, :] = cotangent[:, part].T

    def path_done(step):
        done = path_copy(step, False)
        done.wait_recv()
        done.wait_send()

    loop(1, count, path_done)
    scalars = pltpu.make_async_copy(all_paths, path, local_sem.at[1])
    scalars.start()
    scalars.wait()

    def route(document, column):
        return path[document, 0, column]

    def member_copy(index, source, target, p, landing_own):
        landing = me if landing_own else p
        return pltpu.make_async_remote_copy(
            src_ref=source.at[p],
            dst_ref=target.at[landing],
            send_sem=mem_send.at[index, p],
            recv_sem=mem_recv.at[index, landing],
            device_id={"mem": p},
            device_id_type=MESH,
        )

    def spread(index, source, target):
        loop(
            1,
            members,
            lambda step: member_copy(
                index, source, target, lax.rem(me + step, members), True
            ).start(),
        )

    def arrive(index, source, target):
        loop(
            1,
            members,
            lambda step: member_copy(
                index, source, target, lax.rem(me + members - step, members), False
            ).wait_recv(),
        )

    def left(index, source, target):
        loop(
            1,
            members,
            lambda step: member_copy(
                index, source, target, lax.rem(me + step, members), False
            ).wait_send(),
        )

    def group_copy(index, source, target, step, landing_own):
        other = lax.rem(group + step, groups)
        landing = group if landing_own else other
        return pltpu.make_async_remote_copy(
            src_ref=source(other),
            dst_ref=target.at[landing],
            send_sem=grp_send.at[index, other],
            recv_sem=grp_recv.at[index, landing],
            device_id={"grp": other},
            device_id_type=MESH,
        )

    def group_spread(*what):
        loop(1, groups, lambda step: group_copy(*what, step, True).start())

    def group_arrive(*what):
        loop(1, groups, lambda step: group_copy(*what, step, False).wait_recv())

    def group_left(*what):
        loop(1, groups, lambda step: group_copy(*what, step, False).wait_send())

    def team_copy(index, source, target, step, landing_own):
        other = lax.rem(spot + step, size)
        landing = spot if landing_own else other
        return pltpu.make_async_remote_copy(
            src_ref=source(other),
            dst_ref=target(landing),
            send_sem=team_send.at[index, other],
            recv_sem=team_recv.at[index, landing],
            device_id=(team_first + other // inner, line * inner + lax.rem(other, inner)),
            device_id_type=MESH,
        )

    def team_document(t):
        return (team_first + t // inner) * members + line * inner + lax.rem(t, inner)

    def pick_fine(index):
        held = jnp.clip(route(index, 2) - group * owned, 0, owned - 1)
        fine_out[index // members, lax.rem(index, members)] = fine_w[held]

    def pick_middle(p):
        middle_send[p] = middle_w[route(group * members + p, 1)]

    loop(0, count, pick_fine)
    fine_trade = (0, lambda other: fine_out.at[other], fine_in)
    group_spread(*fine_trade)
    loop(0, members, pick_middle)
    spread(0, middle_send, middle_block)
    fine_in[group] = fine_out[group]
    middle_block[me] = middle_send[me]

    def merge_fine(p):
        owner = route(group * members + p, 2) // owned
        fine_send[p] = fine_in[owner, p]

    group_arrive(*fine_trade)
    loop(0, members, merge_fine)
    spread(1, fine_send, fine_block)
    fine_block[me] = fine_send[me]

    line_self.wait()
    loop(1, outer, lambda step: line_copy(*first_stage, step, False).wait_recv())

    def pick_coarse(t):
        identity = route(team_document(t), 0)
        for z in range(outer):
            coarse_send[t, z] = coarse_line[z, identity]

    loop(0, size, pick_coarse)

    def piece_of(ref, t, s):
        return ref.at[:, lax.rem(t, inner), :, column_range(s)]

    second_stage = (
        0,
        lambda other: coarse_send.at[other],
        lambda landing: piece_of(coarse_block, landing, landing // inner),
    )
    loop(1, size, lambda step: team_copy(*second_stage, step, True).start())
    block_self = pltpu.make_async_copy(
        coarse_send.at[spot], piece_of(coarse_block, place, slot), local_sem.at[2]
    )
    block_self.start()

    def compute(block, term):
        weights = block[...].reshape(width, block.shape[-1])
        value, part = level(weights, tokens[...], cotangent[...], xt[...], gt[...])
        term[...] = value.reshape(term.shape)
        return part

    middle_own = middle_parts.at[group]
    fine_own = fine_parts.at[group]

    loop(1, size, lambda step: team_copy(*second_stage, step, False).wait_recv())
    block_self.wait()
    total[...] = compute(coarse_block, coarse_term)
    gather_terms = (
        1,
        lambda other: piece_of(coarse_term, other, other // inner),
        lambda landing: coarse_terms_in.at[landing],
    )
    loop(1, size, lambda step: team_copy(*gather_terms, step, True).start())
    term_self = pltpu.make_async_copy(
        piece_of(coarse_term, place, slot), coarse_terms_in.at[spot], local_sem.at[3]
    )
    term_self.start()

    arrive(0, middle_send, middle_block)
    total[...] += compute(middle_block, middle_term)
    spread(2, middle_term, middle_own)
    middle_parts[group, me] = middle_term[me]

    arrive(1, fine_send, fine_block)
    part = compute(fine_block, fine_term)
    spread(3, fine_term, fine_own)
    fine_parts[group, me] = fine_term[me]
    tokens_grad[...] = (total[...] + part).astype(BF16)

    loop(1, size, lambda step: team_copy(*gather_terms, step, False).wait_recv())
    term_self.wait()
    step_rows = min(rows, 16)
    weight = [
        [jnp.where(route(team_document(t), 0) == k, 1.0, 0.0) for k in range(coarse_count)]
        for t in range(size)
    ]

    def add_terms(index):
        z = index // (rows // step_rows)
        some = pl.ds(pl.multiple_of(lax.rem(index, rows // step_rows) * step_rows, step_rows), step_rows)
        pieces = [coarse_terms_in[t, z, some, :].astype(F32) for t in range(size)]
        for k in range(coarse_count):
            value = pieces[0] * weight[0][k]
            for t in range(1, size):
                value = value + pieces[t] * weight[t][k]
            coarse_sums[z, k, some, :] = value.astype(BF16)

    loop(0, outer * (rows // step_rows), add_terms)
    sum_stage = (1, lambda other: coarse_sums.at[other], coarse_sums_in)
    loop(1, outer, lambda step: line_copy(*sum_stage, step, True).start())
    coarse_sums_in[line] = coarse_sums[line]

    arrive(2, middle_term, middle_own)
    middle_trade = (1, lambda other: middle_own, middle_parts)
    group_spread(*middle_trade)
    arrive(3, fine_term, fine_own)
    fine_trade_back = (2, lambda other: fine_own, fine_parts)
    group_spread(*fine_trade_back)

    left(0, middle_send, middle_block)
    left(1, fine_send, fine_block)
    group_left(*fine_trade)
    loop(1, outer, lambda step: line_copy(*first_stage, step, False).wait_send())
    loop(1, size, lambda step: team_copy(*second_stage, step, False).wait_send())
    loop(1, size, lambda step: team_copy(*gather_terms, step, False).wait_send())
    left(2, middle_term, middle_own)
    left(3, fine_term, fine_own)

    loop(1, outer, lambda step: line_copy(*sum_stage, step, False).wait_recv())
    value = coarse_sums_in[0].astype(F32)
    for z in range(1, outer):
        value = value + coarse_sums_in[z].astype(F32)
    coarse_total[...] = value.astype(BF16)
    coarse_trade = (3, lambda other: coarse_total, coarse_parts)
    group_spread(*coarse_trade)
    coarse_parts[group] = coarse_total[...]
    loop(1, outer, lambda step: line_copy(*sum_stage, step, False).wait_send())
    for trade in (middle_trade, fine_trade_back, coarse_trade):
        group_arrive(*trade)
        group_left(*trade)


def exchange(path, tokens, cotangent, coarse_w, middle_w, fine_w, groups, members):
    blocks, rows, wide = coarse_w.shape
    medium, narrow = middle_w.shape[2], fine_w.shape[2]
    token_count, width = tokens.shape
    count = groups * members
    outer, inner, team = plan(groups, members, wide)
    columns = wide // team
    size = team * inner

    def stack(*shape):
        return pltpu.VMEM(shape, BF16)

    def sems(*shape):
        return pltpu.SemaphoreType.DMA(shape)

    vmem = pl.BlockSpec(memory_space=pltpu.VMEM)
    return pl.pallas_call(
        functools.partial(main_kernel, groups, members),
        out_shape=(
            jax.ShapeDtypeStruct((count,) + path.shape, jnp.int32),
            jax.ShapeDtypeStruct(tokens.shape, BF16),
            jax.ShapeDtypeStruct((groups, members, rows, medium), BF16),
            jax.ShapeDtypeStruct((groups, members, rows, narrow), BF16),
            jax.ShapeDtypeStruct((groups, blocks, rows, columns), BF16),
        ),
        in_specs=[vmem] * 6,
        out_specs=(vmem,) * 5,
        scratch_shapes=[
            pltpu.SMEM((count,) + path.shape, jnp.int32),
            stack(members, rows, medium),
            stack(groups, members, rows, narrow),
            stack(groups, members, rows, narrow),
            stack(members, rows, narrow),
            stack(outer, blocks, rows, columns),
            stack(size, outer, rows, columns),
            stack(outer, inner, rows, wide),
            stack(members, rows, medium),
            stack(members, rows, narrow),
            stack(outer, inner, rows, wide),
            stack(members, rows, medium),
            stack(members, rows, narrow),
            stack(size, outer, rows, columns),
            stack(outer, blocks, rows, columns),
            stack(outer, blocks, rows, columns),
            stack(blocks, rows, columns),
            stack(width, token_count),
            stack(width, token_count),
            pltpu.VMEM((token_count, width), F32),
            sems(count),
            sems(count),
            sems(4, members),
            sems(4, members),
            sems(4, groups),
            sems(4, groups),
            sems(2, outer),
            sems(2, outer),
            sems(2, size),
            sems(2, size),
            sems(4),
        ],
        compiler_params=pltpu.CompilerParams(
            collective_id=0, has_side_effects=True, vmem_limit_bytes=60 * 2**20
        ),
        name="exchange",
    )(path, tokens, cotangent, coarse_w, middle_w, fine_w)


def collect_kernel(
    path,
    first_owned,
    middle_parts,
    fine_parts,
    coarse_parts,
    coarse_grad,
    middle_grad,
    fine_grad,
    middle_sum,
    fine_sum,
):
    owned = fine_grad.shape[0]
    middle_sum[...] = jnp.zeros_like(middle_sum)
    fine_sum[...] = jnp.zeros_like(fine_sum)

    def add(document, carry):
        k = path[document, 0, 1]
        middle_sum[k] += middle_parts[document].astype(F32)
        place = path[document, 0, 2] - first_owned[0]

        @pl.when((place >= 0) & (place < owned))
        def _():
            fine_sum[place] += fine_parts[document].astype(F32)

        return carry

    lax.fori_loop(0, middle_parts.shape[0], add, 0)
    middle_grad[...] = middle_sum[...].astype(BF16)
    fine_grad[...] = fine_sum[...].astype(BF16)
    groups, _, _, columns = coarse_parts.shape
    team = coarse_grad.shape[2] // columns
    for s in range(team):
        value = coarse_parts[s].astype(F32)
        for other in range(s + team, groups, team):
            value = value + coarse_parts[other].astype(F32)
        coarse_grad[:, :, s * columns : (s + 1) * columns] = value.astype(BF16)


def collect(paths, first_owned, middle_parts, fine_parts, coarse_parts, shapes):
    vmem = pl.BlockSpec(memory_space=pltpu.VMEM)
    smem = pl.BlockSpec(memory_space=pltpu.SMEM)
    return pl.pallas_call(
        collect_kernel,
        out_shape=tuple(jax.ShapeDtypeStruct(shape, BF16) for shape in shapes),
        in_specs=[smem, smem] + [vmem] * 3,
        out_specs=(vmem,) * 3,
        scratch_shapes=[pltpu.VMEM(shapes[1], F32), pltpu.VMEM(shapes[2], F32)],
        compiler_params=pltpu.CompilerParams(vmem_limit_bytes=60 * 2**20),
        name="collect",
    )(paths, first_owned, middle_parts, fine_parts, coarse_parts)


def on_device(tokens, cotangent, path, coarse_weights, middle_weights, fine_weights):
    members = lax.axis_size("mem")
    groups = lax.axis_size("grp")
    paths, tokens_grad, middle_parts, fine_parts, coarse_parts = exchange(
        path, tokens, cotangent, coarse_weights, middle_weights, fine_weights, groups, members
    )
    first_owned = (lax.axis_index("grp") * fine_weights.shape[0]).astype(jnp.int32).reshape(1)
    flat = lambda parts: parts.reshape((groups * members,) + parts.shape[2:])
    grads = collect(
        paths,
        first_owned,
        flat(middle_parts),
        flat(fine_parts),
        coarse_parts,
        (coarse_weights.shape, middle_weights.shape, fine_weights.shape),
    )
    return (tokens_grad,) + tuple(grads)


def solution(mesh):
    return jax.shard_map(
        on_device,
        mesh=mesh,
        in_specs=(
            P(("grp", "mem"), None),
            P(("grp", "mem"), None),
            P(("grp", "mem"), None),
            P(None, "mem", None),
            P(None, "mem", None),
            P("grp", "mem", None),
        ),
        out_specs=(
            P(("grp", "mem"), None),
            P(None, "mem", None),
            P(None, "mem", None),
            P("grp", "mem", None),
        ),
        check_vma=False,
    )
```

```python
import functools
import math

import jax
import jax.numpy as jnp
from jax import lax
from jax.experimental import pallas as pl
from jax.experimental.pallas import tpu as pltpu
from jax.sharding import PartitionSpec as P

MESH = pl.DeviceIdType.MESH
LANES = 128
F32 = jnp.float32
BF16 = jnp.bfloat16


def gelu_parts(before, hidden_grad):
    scale = math.sqrt(2.0 / math.pi)
    square = before * before
    tanh = jnp.tanh(scale * (before + 0.044715 * (square * before)))
    half = 0.5 * (1.0 + tanh)
    hidden = before * half
    slope = half + 0.5 * before * (1.0 - tanh * tanh) * (scale * (1.0 + 3 * 0.044715 * square))
    return hidden.astype(BF16), (hidden_grad * slope).astype(BF16)


def dot(left, right):
    return jnp.dot(left, right, preferred_element_type=F32)


def dot_transposed(left, right):
    return lax.dot_general(left, right, (((1,), (1,)), ((), ())), preferred_element_type=F32)


def level(weights, x, g, xt, gt):
    width = weights.shape[1]
    half = width // 2
    if half % LANES == 0:
        up = weights[:, :half]
        down = weights[:, half:]
        hidden, grad = gelu_parts(dot(x, up), dot(g, down))
        term = jnp.concatenate(
            [dot(xt, grad).astype(BF16), dot(gt, hidden).astype(BF16)], axis=1
        )
        return term, dot_transposed(grad, up)
    before = dot(x, weights)
    hidden_grad = pltpu.roll(dot(g, weights), half, 1)
    hidden, grad = gelu_parts(before, hidden_grad)
    first = lax.broadcasted_iota(jnp.int32, grad.shape, 1) < half
    grad = jnp.where(first, grad.astype(F32), 0.0).astype(BF16)
    hidden = jnp.where(first, hidden.astype(F32), 0.0)
    hidden = pltpu.roll(hidden, half, 1).astype(BF16)
    term = (dot(xt, grad) + dot(gt, hidden)).astype(BF16)
    return term, dot_transposed(grad, weights)


def plan(groups, members, blocks_width):
    inner = max(k for k in range(1, math.isqrt(members) + 1) if members % k == 0)
    team = math.gcd(groups, blocks_width // LANES)
    return members // inner, inner, team


def main_kernel(
    groups,
    members,
    path_row,
    tokens_hbm,
    cotangent_hbm,
    coarse_hbm,
    middle_hbm,
    fine_hbm,
    all_paths,
    tokens_grad,
    middle_parts,
    fine_parts,
    coarse_parts,
    path,
    tokens,
    cotangent,
    coarse_w,
    middle_w,
    fine_w,
    middle_send,
    fine_out,
    fine_in,
    fine_send,
    coarse_line,
    coarse_send,
    coarse_block,
    middle_block,
    fine_block,
    coarse_term,
    middle_term,
    fine_term,
    coarse_terms_in,
    coarse_sums,
    coarse_sums_in,
    coarse_total,
    xt,
    gt,
    total,
    path_send,
    path_recv,
    mem_send,
    mem_recv,
    grp_send,
    grp_recv,
    line_send,
    line_recv,
    team_send,
    team_recv,
    local_sem,
    load_sem,
    middle_send_on,
    middle_recv_on,
    fine_send_on,
    fine_recv_on,
):
    group = lax.axis_index("grp")
    me = lax.axis_index("mem")
    count = groups * members
    device = group * members + me
    owned = fine_w.shape[0]
    coarse_count, rows, wide = coarse_w.shape
    outer, inner, team = plan(groups, members, wide)
    size = team * inner
    columns = wide // team
    line = me // inner
    place = lax.rem(me, inner)
    slot = lax.rem(group, team)
    team_first = group - slot
    spot = slot * inner + place

    def loop(start, stop, body):
        def wrapped(step, carry):
            body(step)
            return carry

        lax.fori_loop(start, stop, wrapped, 0)

    def column_range(s):
        return pl.ds(pl.multiple_of(s * columns, LANES), columns)

    loads = [
        pltpu.make_async_copy(source, target, load_sem.at[index])
        for index, (source, target) in enumerate(
            (
                (coarse_hbm, coarse_w),
                (fine_hbm, fine_w),
                (middle_hbm, middle_w),
                (tokens_hbm, tokens),
                (cotangent_hbm, cotangent),
            )
        )
    ]
    for load in loads:
        load.start()
    barrier = pltpu.get_barrier_semaphore()

    def anyone(step):
        other = lax.rem(device + step, count)
        return other, (other // members, lax.rem(other, members))

    def greet(step):
        _, where = anyone(step)
        pl.semaphore_signal(barrier, inc=1, device_id=where, device_id_type=MESH)

    loop(1, count, greet)
    own_columns = coarse_w.at[:, :, column_range(slot)]
    loads[0].wait()
    line_self = pltpu.make_async_copy(own_columns, coarse_line.at[line], local_sem.at[0])
    line_self.start()
    pl.semaphore_wait(barrier, count - 1)

    def path_copy(step, landing_own):
        other, where = anyone(step)
        return pltpu.make_async_remote_copy(
            src_ref=path_row,
            dst_ref=all_paths.at[device if landing_own else other],
            send_sem=path_send.at[other],
            recv_sem=path_recv.at[device if landing_own else other],
            device_id=where,
            device_id_type=MESH,
        )

    loop(1, count, lambda step: path_copy(step, True).start())
    all_paths[device] = path_row[...]

    def line_copy(index, source, target, step, landing_own):
        other = lax.rem(line + step, outer)
        landing = line if landing_own else other
        return pltpu.make_async_remote_copy(
            src_ref=source(other),
            dst_ref=target.at[landing],
            send_sem=line_send.at[index, other],
            recv_sem=line_recv.at[index, landing],
            device_id={"mem": other * inner + place},
            device_id_type=MESH,
        )

    first_stage = (0, lambda other: own_columns, coarse_line)
    loop(1, outer, lambda step: line_copy(*first_stage, step, True).start())

    for load in loads[1:]:
        load.wait()
    width = tokens.shape[1]
    for start in range(0, width, LANES):
        part = slice(start, start + LANES)
        xt[part, :] = tokens[:, part].T
        gt[part, :] = cotangent[:, part].T

    def path_done(step):
        done = path_copy(step, False)
        done.wait_recv()
        done.wait_send()

    loop(1, count, path_done)
    scalars = pltpu.make_async_copy(all_paths, path, local_sem.at[1])
    scalars.start()
    scalars.wait()

    def route(document, column):
        return path[document, 0, column]

    def member_copy(index, source, target, p, landing_own):
        landing = me if landing_own else p
        return pltpu.make_async_remote_copy(
            src_ref=source.at[p],
            dst_ref=target.at[landing],
            send_sem=mem_send.at[index, p],
            recv_sem=mem_recv.at[index, landing],
            device_id={"mem": p},
            device_id_type=MESH,
        )

    def spread(index, source, target):
        loop(
            1,
            members,
            lambda step: member_copy(
                index, source, target, lax.rem(me + step, members), True
            ).start(),
        )

    def arrive(index, source, target):
        loop(
            1,
            members,
            lambda step: member_copy(
                index, source, target, lax.rem(me + members - step, members), False
            ).wait_recv(),
        )

    def left(index, source, target):
        loop(
            1,
            members,
            lambda step: member_copy(
                index, source, target, lax.rem(me + step, members), False
            ).wait_send(),
        )

    def group_copy(index, source, target, step, landing_own):
        other = lax.rem(group + step, groups)
        landing = group if landing_own else other
        return pltpu.make_async_remote_copy(
            src_ref=source(other),
            dst_ref=target.at[landing],
            send_sem=grp_send.at[index, other],
            recv_sem=grp_recv.at[index, landing],
            device_id={"grp": other},
            device_id_type=MESH,
        )

    def group_spread(*what):
        loop(1, groups, lambda step: group_copy(*what, step, True).start())

    def group_arrive(*what):
        loop(1, groups, lambda step: group_copy(*what, step, False).wait_recv())

    def group_left(*what):
        loop(1, groups, lambda step: group_copy(*what, step, False).wait_send())

    def team_copy(index, source, target, step, landing_own):
        other = lax.rem(spot + step, size)
        landing = spot if landing_own else other
        return pltpu.make_async_remote_copy(
            src_ref=source(other),
            dst_ref=target(landing),
            send_sem=team_send.at[index, other],
            recv_sem=team_recv.at[index, landing],
            device_id=(team_first + other // inner, line * inner + lax.rem(other, inner)),
            device_id_type=MESH,
        )

    def team_document(t):
        return (team_first + t // inner) * members + line * inner + lax.rem(t, inner)

    def pick_fine(index):
        held = jnp.clip(route(index, 2) - group * owned, 0, owned - 1)
        fine_out[index // members, lax.rem(index, members)] = fine_w[held]

    def pick_middle(p):
        middle_send[p] = middle_w[route(group * members + p, 1)]

    loop(0, count, pick_fine)
    fine_trade = (0, lambda other: fine_out.at[other], fine_in)
    group_spread(*fine_trade)
    loop(0, members, pick_middle)
    spread(0, middle_send, middle_block)
    fine_in[group] = fine_out[group]
    middle_block[me] = middle_send[me]

    def merge_fine(p):
        owner = route(group * members + p, 2) // owned
        fine_send[p] = fine_in[owner, p]

    group_arrive(*fine_trade)
    loop(0, members, merge_fine)
    spread(1, fine_send, fine_block)
    fine_block[me] = fine_send[me]

    line_self.wait()
    loop(1, outer, lambda step: line_copy(*first_stage, step, False).wait_recv())

    def pick_coarse(t):
        identity = route(team_document(t), 0)
        for z in range(outer):
            coarse_send[t, z] = coarse_line[z, identity]

    loop(0, size, pick_coarse)

    def piece_of(ref, t, s):
        return ref.at[:, lax.rem(t, inner), :, column_range(s)]

    second_stage = (
        0,
        lambda other: coarse_send.at[other],
        lambda landing: piece_of(coarse_block, landing, landing // inner),
    )
    loop(1, size, lambda step: team_copy(*second_stage, step, True).start())
    block_self = pltpu.make_async_copy(
        coarse_send.at[spot], piece_of(coarse_block, place, slot), local_sem.at[2]
    )
    block_self.start()

    def compute(block, term):
        weights = block[...].reshape(width, block.shape[-1])
        value, part = level(weights, tokens[...], cotangent[...], xt[...], gt[...])
        term[...] = value.reshape(term.shape)
        return part

    middle_own = middle_parts.at[group]
    fine_own = fine_parts.at[group]

    loop(1, size, lambda step: team_copy(*second_stage, step, False).wait_recv())
    block_self.wait()
    total[...] = compute(coarse_block, coarse_term)
    gather_terms = (
        1,
        lambda other: piece_of(coarse_term, other, other // inner),
        lambda landing: coarse_terms_in.at[landing],
    )
    loop(1, size, lambda step: team_copy(*gather_terms, step, True).start())
    term_self = pltpu.make_async_copy(
        piece_of(coarse_term, place, slot), coarse_terms_in.at[spot], local_sem.at[3]
    )
    term_self.start()

    arrive(0, middle_send, middle_block)
    total[...] += compute(middle_block, middle_term)
    spread(2, middle_term, middle_own)
    middle_parts[group, me] = middle_term[me]

    arrive(1, fine_send, fine_block)
    part = compute(fine_block, fine_term)
    spread(3, fine_term, fine_own)
    fine_parts[group, me] = fine_term[me]
    tokens_grad[...] = (total[...] + part).astype(BF16)

    def hand_on(target, send_on, recv_on, p, step, landing_own):
        other = lax.rem(group + step, groups)
        landing = group if landing_own else other
        return pltpu.make_async_remote_copy(
            src_ref=target.at[group, p],
            dst_ref=target.at[landing, p],
            send_sem=send_on.at[other, p],
            recv_sem=recv_on.at[landing, p],
            device_id={"grp": other},
            device_id_type=MESH,
        )

    def relay(index, source, target, send_on, recv_on):
        own = target.at[group]

        def start(p):
            loop(1, groups, lambda step: hand_on(target, send_on, recv_on, p, step, True).start())

        def body(step):
            p = lax.rem(me + members - step, members)
            member_copy(index, source, own, p, False).wait_recv()
            start(p)

        start(me)
        loop(1, members, body)

    def relay_done(target, send_on, recv_on):
        def body(index):
            p = index // (groups - 1)
            step = lax.rem(index, groups - 1) + 1
            done = hand_on(target, send_on, recv_on, p, step, False)
            done.wait_recv()
            done.wait_send()

        if groups > 1:
            loop(0, members * (groups - 1), body)

    loop(1, size, lambda step: team_copy(*gather_terms, step, False).wait_recv())
    term_self.wait()
    step_rows = min(rows, 16)
    weight = [
        [jnp.where(route(team_document(t), 0) == k, 1.0, 0.0) for k in range(coarse_count)]
        for t in range(size)
    ]

    def add_terms(index):
        z = index // (rows // step_rows)
        some = pl.ds(pl.multiple_of(lax.rem(index, rows // step_rows) * step_rows, step_rows), step_rows)
        pieces = [coarse_terms_in[t, z, some, :].astype(F32) for t in range(size)]
        for k in range(coarse_count):
            value = pieces[0] * weight[0][k]
            for t in range(1, size):
                value = value + pieces[t] * weight[t][k]
            coarse_sums[z, k, some, :] = value.astype(BF16)

    loop(0, outer * (rows // step_rows), add_terms)
    sum_stage = (1, lambda other: coarse_sums.at[other], coarse_sums_in)
    loop(1, outer, lambda step: line_copy(*sum_stage, step, True).start())
    coarse_sums_in[line] = coarse_sums[line]
    relay(2, middle_term, middle_parts, middle_send_on, middle_recv_on)
    relay(3, fine_term, fine_parts, fine_send_on, fine_recv_on)


    left(0, middle_send, middle_block)
    left(1, fine_send, fine_block)
    group_left(*fine_trade)
    loop(1, outer, lambda step: line_copy(*first_stage, step, False).wait_send())
    loop(1, size, lambda step: team_copy(*second_stage, step, False).wait_send())
    loop(1, size, lambda step: team_copy(*gather_terms, step, False).wait_send())
    left(2, middle_term, middle_own)
    left(3, fine_term, fine_own)

    loop(1, outer, lambda step: line_copy(*sum_stage, step, False).wait_recv())
    value = coarse_sums_in[0].astype(F32)
    for z in range(1, outer):
        value = value + coarse_sums_in[z].astype(F32)
    coarse_total[...] = value.astype(BF16)
    coarse_trade = (1, lambda other: coarse_total, coarse_parts)
    group_spread(*coarse_trade)
    coarse_parts[group] = coarse_total[...]
    loop(1, outer, lambda step: line_copy(*sum_stage, step, False).wait_send())
    group_arrive(*coarse_trade)
    group_left(*coarse_trade)
    relay_done(middle_parts, middle_send_on, middle_recv_on)
    relay_done(fine_parts, fine_send_on, fine_recv_on)


def exchange(path, tokens, cotangent, coarse_w, middle_w, fine_w, groups, members):
    blocks, rows, wide = coarse_w.shape
    medium, narrow = middle_w.shape[2], fine_w.shape[2]
    token_count, width = tokens.shape
    count = groups * members
    outer, inner, team = plan(groups, members, wide)
    columns = wide // team
    size = team * inner

    def stack(*shape):
        return pltpu.VMEM(shape, BF16)

    def sems(*shape):
        return pltpu.SemaphoreType.DMA(shape)

    vmem = pl.BlockSpec(memory_space=pltpu.VMEM)
    return pl.pallas_call(
        functools.partial(main_kernel, groups, members),
        out_shape=(
            jax.ShapeDtypeStruct((count,) + path.shape, jnp.int32),
            jax.ShapeDtypeStruct(tokens.shape, BF16),
            jax.ShapeDtypeStruct((groups, members, rows, medium), BF16),
            jax.ShapeDtypeStruct((groups, members, rows, narrow), BF16),
            jax.ShapeDtypeStruct((groups, blocks, rows, columns), BF16),
        ),
        in_specs=[vmem] + [pl.BlockSpec(memory_space=pl.ANY)] * 5,
        out_specs=(vmem,) * 5,
        scratch_shapes=[
            pltpu.SMEM((count,) + path.shape, jnp.int32),
            stack(*tokens.shape),
            stack(*cotangent.shape),
            stack(*coarse_w.shape),
            stack(*middle_w.shape),
            stack(*fine_w.shape),
            stack(members, rows, medium),
            stack(groups, members, rows, narrow),
            stack(groups, members, rows, narrow),
            stack(members, rows, narrow),
            stack(outer, blocks, rows, columns),
            stack(size, outer, rows, columns),
            stack(outer, inner, rows, wide),
            stack(members, rows, medium),
            stack(members, rows, narrow),
            stack(outer, inner, rows, wide),
            stack(members, rows, medium),
            stack(members, rows, narrow),
            stack(size, outer, rows, columns),
            stack(outer, blocks, rows, columns),
            stack(outer, blocks, rows, columns),
            stack(blocks, rows, columns),
            stack(width, token_count),
            stack(width, token_count),
            pltpu.VMEM((token_count, width), F32),
            sems(count),
            sems(count),
            sems(4, members),
            sems(4, members),
            sems(2, groups),
            sems(2, groups),
            sems(2, outer),
            sems(2, outer),
            sems(2, size),
            sems(2, size),
            sems(4),
            sems(5),
            sems(groups, members),
            sems(groups, members),
            sems(groups, members),
            sems(groups, members),
        ],
        compiler_params=pltpu.CompilerParams(
            collective_id=0, has_side_effects=True, vmem_limit_bytes=60 * 2**20
        ),
        name="exchange",
    )(path, tokens, cotangent, coarse_w, middle_w, fine_w)


def collect_kernel(
    path,
    first_owned,
    tokens_in,
    middle_hbm,
    fine_hbm,
    coarse_parts,
    tokens_grad,
    coarse_grad,
    middle_grad,
    fine_grad,
    middle_parts,
    fine_parts,
    middle_sum,
    fine_sum,
    middle_last,
    fine_last,
    load_sem,
):
    count = middle_parts.shape[0]
    owned = fine_grad.shape[0]
    loads = (
        pltpu.make_async_copy(middle_hbm, middle_parts, load_sem.at[0]),
        pltpu.make_async_copy(fine_hbm, fine_parts, load_sem.at[1]),
    )
    for load in loads:
        load.start()
    middle_grad[...] = jnp.zeros_like(middle_grad)
    fine_grad[...] = jnp.zeros_like(fine_grad)
    middle_sum[count] = jnp.zeros(middle_sum.shape[1:], F32)
    fine_sum[count] = jnp.zeros(fine_sum.shape[1:], F32)
    for last in (middle_last, fine_last):

        def clear(k, carry, last=last):
            last[k] = count
            return carry

        lax.fori_loop(0, last.shape[0], clear, 0)
    tokens_grad[...] = tokens_in[...]
    groups, _, _, columns = coarse_parts.shape
    team = coarse_grad.shape[2] // columns
    for s in range(team):
        value = coarse_parts[s].astype(F32)
        for other in range(s + team, groups, team):
            value = value + coarse_parts[other].astype(F32)
        coarse_grad[:, :, s * columns : (s + 1) * columns] = value.astype(BF16)
    for load in loads:
        load.wait()

    def add(document, carry):
        k = path[document, 0, 1]
        value = middle_parts[document].astype(F32) + middle_sum[middle_last[k]]
        middle_sum[document] = value
        middle_grad[k] = value.astype(BF16)
        middle_last[k] = document
        place = path[document, 0, 2] - first_owned[0]

        @pl.when((place >= 0) & (place < owned))
        def _():
            piece = fine_parts[document].astype(F32) + fine_sum[fine_last[place]]
            fine_sum[document] = piece
            fine_grad[place] = piece.astype(BF16)
            fine_last[place] = document

        return carry

    lax.fori_loop(0, count, add, 0)


def collect(paths, first_owned, tokens_grad, middle_parts, fine_parts, coarse_parts, shapes):
    vmem = pl.BlockSpec(memory_space=pltpu.VMEM)
    smem = pl.BlockSpec(memory_space=pltpu.SMEM)
    hbm = pl.BlockSpec(memory_space=pl.ANY)
    count, rows, medium = middle_parts.shape
    narrow = fine_parts.shape[2]
    return pl.pallas_call(
        collect_kernel,
        out_shape=tuple(
            jax.ShapeDtypeStruct(shape, BF16) for shape in (tokens_grad.shape,) + shapes
        ),
        in_specs=[smem, smem, vmem, hbm, hbm, vmem],
        out_specs=(vmem,) * 4,
        scratch_shapes=[
            pltpu.VMEM(middle_parts.shape, BF16),
            pltpu.VMEM(fine_parts.shape, BF16),
            pltpu.VMEM((count + 1, rows, medium), F32),
            pltpu.VMEM((count + 1, rows, narrow), F32),
            pltpu.SMEM((shapes[1][0],), jnp.int32),
            pltpu.SMEM((shapes[2][0],), jnp.int32),
            pltpu.SemaphoreType.DMA((2,)),
        ],
        compiler_params=pltpu.CompilerParams(vmem_limit_bytes=60 * 2**20),
        name="collect",
    )(paths, first_owned, tokens_grad, middle_parts, fine_parts, coarse_parts)


def on_device(tokens, cotangent, path, coarse_weights, middle_weights, fine_weights):
    members = lax.axis_size("mem")
    groups = lax.axis_size("grp")
    paths, tokens_grad, middle_parts, fine_parts, coarse_parts = exchange(
        path, tokens, cotangent, coarse_weights, middle_weights, fine_weights, groups, members
    )
    first_owned = (lax.axis_index("grp") * fine_weights.shape[0]).astype(jnp.int32).reshape(1)
    flat = lambda parts: parts.reshape((groups * members,) + parts.shape[2:])
    return collect(
        paths,
        first_owned,
        tokens_grad,
        flat(middle_parts),
        flat(fine_parts),
        coarse_parts,
        (coarse_weights.shape, middle_weights.shape, fine_weights.shape),
    )


def solution(mesh):
    return jax.shard_map(
        on_device,
        mesh=mesh,
        in_specs=(
            P(("grp", "mem"), None),
            P(("grp", "mem"), None),
            P(("grp", "mem"), None),
            P(None, "mem", None),
            P(None, "mem", None),
            P("grp", "mem", None),
        ),
        out_specs=(
            P(("grp", "mem"), None),
            P(None, "mem", None),
            P(None, "mem", None),
            P("grp", "mem", None),
        ),
        check_vma=False,
    )
```

```python
import functools
import math

import jax
import jax.numpy as jnp
from jax import lax
from jax.experimental import pallas as pl
from jax.experimental.pallas import tpu as pltpu
from jax.sharding import PartitionSpec as P

MESH = pl.DeviceIdType.MESH
LANES = 128
F32 = jnp.float32
BF16 = jnp.bfloat16


def gelu_parts(before, hidden_grad):
    scale = math.sqrt(2.0 / math.pi)
    square = before * before
    tanh = jnp.tanh(scale * (before + 0.044715 * (square * before)))
    half = 0.5 * (1.0 + tanh)
    hidden = before * half
    slope = half + 0.5 * before * (1.0 - tanh * tanh) * (scale * (1.0 + 3 * 0.044715 * square))
    return hidden.astype(BF16), (hidden_grad * slope).astype(BF16)


def dot(left, right):
    return jnp.dot(left, right, preferred_element_type=F32)


def dot_transposed(left, right):
    return lax.dot_general(left, right, (((1,), (1,)), ((), ())), preferred_element_type=F32)


def level(weights, x, g, xt, gt):
    width = weights.shape[1]
    half = width // 2
    if half % LANES == 0:
        up = weights[:, :half]
        down = weights[:, half:]
        hidden, grad = gelu_parts(dot(x, up), dot(g, down))
        term = jnp.concatenate(
            [dot(xt, grad).astype(BF16), dot(gt, hidden).astype(BF16)], axis=1
        )
        return term, dot_transposed(grad, up)
    before = dot(x, weights)
    hidden_grad = pltpu.roll(dot(g, weights), half, 1)
    hidden, grad = gelu_parts(before, hidden_grad)
    first = lax.broadcasted_iota(jnp.int32, grad.shape, 1) < half
    grad = jnp.where(first, grad.astype(F32), 0.0).astype(BF16)
    hidden = jnp.where(first, hidden.astype(F32), 0.0)
    hidden = pltpu.roll(hidden, half, 1).astype(BF16)
    term = (dot(xt, grad) + dot(gt, hidden)).astype(BF16)
    return term, dot_transposed(grad, weights)


def plan(groups, members, blocks_width):
    inner = max(k for k in range(1, math.isqrt(members) + 1) if members % k == 0)
    team = math.gcd(groups, blocks_width // LANES)
    return members // inner, inner, team


def main_kernel(
    groups,
    members,
    path_row,
    tokens_hbm,
    cotangent_hbm,
    coarse_hbm,
    middle_hbm,
    fine_hbm,
    all_paths,
    tokens_grad,
    middle_parts,
    fine_parts,
    coarse_parts,
    path,
    tokens,
    cotangent,
    coarse_w,
    middle_w,
    fine_w,
    middle_send,
    fine_out,
    fine_in,
    fine_send,
    coarse_line,
    coarse_send,
    coarse_block,
    middle_block,
    fine_block,
    coarse_term,
    middle_term,
    fine_term,
    coarse_terms_in,
    coarse_sums,
    coarse_sums_in,
    coarse_total,
    xt,
    gt,
    total,
    path_send,
    path_recv,
    mem_send,
    mem_recv,
    grp_send,
    grp_recv,
    line_send,
    line_recv,
    team_send,
    team_recv,
    local_sem,
    load_sem,
    middle_send_on,
    middle_recv_on,
    fine_send_on,
    fine_recv_on,
):
    group = lax.axis_index("grp")
    me = lax.axis_index("mem")
    count = groups * members
    device = group * members + me
    owned = fine_w.shape[0]
    coarse_count, rows, wide = coarse_w.shape
    outer, inner, team = plan(groups, members, wide)
    size = team * inner
    columns = wide // team
    line = me // inner
    place = lax.rem(me, inner)
    slot = lax.rem(group, team)
    team_first = group - slot
    spot = slot * inner + place

    def loop(start, stop, body):
        def wrapped(step, carry):
            body(step)
            return carry

        lax.fori_loop(start, stop, wrapped, 0)

    def column_range(s):
        return pl.ds(pl.multiple_of(s * columns, LANES), columns)

    loads = [
        pltpu.make_async_copy(source, target, load_sem.at[index])
        for index, (source, target) in enumerate(
            (
                (coarse_hbm, coarse_w),
                (fine_hbm, fine_w),
                (middle_hbm, middle_w),
                (tokens_hbm, tokens),
                (cotangent_hbm, cotangent),
            )
        )
    ]
    for load in loads:
        load.start()
    barrier = pltpu.get_barrier_semaphore()

    def anyone(step):
        other = lax.rem(device + step, count)
        return other, (other // members, lax.rem(other, members))

    def greet(step):
        _, where = anyone(step)
        pl.semaphore_signal(barrier, inc=1, device_id=where, device_id_type=MESH)

    loop(1, count, greet)
    own_columns = coarse_w.at[:, :, column_range(slot)]
    loads[0].wait()
    line_self = pltpu.make_async_copy(own_columns, coarse_line.at[line], local_sem.at[0])
    line_self.start()
    pl.semaphore_wait(barrier, count - 1)

    def path_copy(step, landing_own):
        other, where = anyone(step)
        return pltpu.make_async_remote_copy(
            src_ref=path_row,
            dst_ref=all_paths.at[device if landing_own else other],
            send_sem=path_send.at[other],
            recv_sem=path_recv.at[device if landing_own else other],
            device_id=where,
            device_id_type=MESH,
        )

    loop(1, count, lambda step: path_copy(step, True).start())
    all_paths[device] = path_row[...]

    def line_copy(index, source, target, step, landing_own):
        other = lax.rem(line + step, outer)
        landing = line if landing_own else other
        return pltpu.make_async_remote_copy(
            src_ref=source(other),
            dst_ref=target.at[landing],
            send_sem=line_send.at[index, other],
            recv_sem=line_recv.at[index, landing],
            device_id={"mem": other * inner + place},
            device_id_type=MESH,
        )

    first_stage = (0, lambda other: own_columns, coarse_line)
    loop(1, outer, lambda step: line_copy(*first_stage, step, True).start())

    for load in loads[1:]:
        load.wait()
    width = tokens.shape[1]
    for start in range(0, width, LANES):
        part = slice(start, start + LANES)
        xt[part, :] = tokens[:, part].T
        gt[part, :] = cotangent[:, part].T

    def path_done(step):
        done = path_copy(step, False)
        done.wait_recv()
        done.wait_send()

    loop(1, count, path_done)
    scalars = pltpu.make_async_copy(all_paths, path, local_sem.at[1])
    scalars.start()
    scalars.wait()

    def route(document, column):
        return path[document, 0, column]

    def member_copy(index, source, target, p, landing_own):
        landing = me if landing_own else p
        return pltpu.make_async_remote_copy(
            src_ref=source.at[p],
            dst_ref=target.at[landing],
            send_sem=mem_send.at[index, p],
            recv_sem=mem_recv.at[index, landing],
            device_id={"mem": p},
            device_id_type=MESH,
        )

    def spread(index, source, target):
        loop(
            1,
            members,
            lambda step: member_copy(
                index, source, target, lax.rem(me + step, members), True
            ).start(),
        )

    def arrive(index, source, target):
        loop(
            1,
            members,
            lambda step: member_copy(
                index, source, target, lax.rem(me + members - step, members), False
            ).wait_recv(),
        )

    def left(index, source, target):
        loop(
            1,
            members,
            lambda step: member_copy(
                index, source, target, lax.rem(me + step, members), False
            ).wait_send(),
        )

    def group_copy(index, source, target, step, landing_own):
        other = lax.rem(group + step, groups)
        landing = group if landing_own else other
        return pltpu.make_async_remote_copy(
            src_ref=source(other),
            dst_ref=target.at[landing],
            send_sem=grp_send.at[index, other],
            recv_sem=grp_recv.at[index, landing],
            device_id={"grp": other},
            device_id_type=MESH,
        )

    def group_spread(*what):
        loop(1, groups, lambda step: group_copy(*what, step, True).start())

    def group_arrive(*what):
        loop(1, groups, lambda step: group_copy(*what, step, False).wait_recv())

    def group_left(*what):
        loop(1, groups, lambda step: group_copy(*what, step, False).wait_send())

    def team_copy(index, source, target, step, landing_own):
        other = lax.rem(spot + step, size)
        landing = spot if landing_own else other
        return pltpu.make_async_remote_copy(
            src_ref=source(other),
            dst_ref=target(landing),
            send_sem=team_send.at[index, other],
            recv_sem=team_recv.at[index, landing],
            device_id=(team_first + other // inner, line * inner + lax.rem(other, inner)),
            device_id_type=MESH,
        )

    def team_document(t):
        return (team_first + t // inner) * members + line * inner + lax.rem(t, inner)

    def pick_fine(index):
        held = jnp.clip(route(index, 2) - group * owned, 0, owned - 1)
        fine_out[index // members, lax.rem(index, members)] = fine_w[held]

    def pick_middle(p):
        middle_send[p] = middle_w[route(group * members + p, 1)]

    loop(0, count, pick_fine)
    fine_trade = (0, lambda other: fine_out.at[other], fine_in)
    group_spread(*fine_trade)
    loop(0, members, pick_middle)
    spread(0, middle_send, middle_block)
    fine_in[group] = fine_out[group]
    middle_block[me] = middle_send[me]

    def merge_fine(p):
        owner = route(group * members + p, 2) // owned
        fine_send[p] = fine_in[owner, p]

    group_arrive(*fine_trade)
    loop(0, members, merge_fine)
    spread(1, fine_send, fine_block)
    fine_block[me] = fine_send[me]

    line_self.wait()
    loop(1, outer, lambda step: line_copy(*first_stage, step, False).wait_recv())

    def pick_coarse(t):
        identity = route(team_document(t), 0)
        for z in range(outer):
            coarse_send[t, z] = coarse_line[z, identity]

    loop(0, size, pick_coarse)

    def piece_of(ref, t, s):
        return ref.at[:, lax.rem(t, inner), :, column_range(s)]

    second_stage = (
        0,
        lambda other: coarse_send.at[other],
        lambda landing: piece_of(coarse_block, landing, landing // inner),
    )
    loop(1, size, lambda step: team_copy(*second_stage, step, True).start())
    block_self = pltpu.make_async_copy(
        coarse_send.at[spot], piece_of(coarse_block, place, slot), local_sem.at[2]
    )
    block_self.start()

    def compute(block, term):
        weights = block[...].reshape(width, block.shape[-1])
        value, part = level(weights, tokens[...], cotangent[...], xt[...], gt[...])
        term[...] = value.reshape(term.shape)
        return part

    middle_own = middle_parts.at[group]
    fine_own = fine_parts.at[group]

    arrive(0, middle_send, middle_block)
    total[...] = compute(middle_block, middle_term)
    spread(2, middle_term, middle_own)
    middle_parts[group, me] = middle_term[me]

    loop(1, size, lambda step: team_copy(*second_stage, step, False).wait_recv())
    block_self.wait()
    total[...] += compute(coarse_block, coarse_term)
    gather_terms = (
        1,
        lambda other: piece_of(coarse_term, other, other // inner),
        lambda landing: coarse_terms_in.at[landing],
    )
    loop(1, size, lambda step: team_copy(*gather_terms, step, True).start())
    term_self = pltpu.make_async_copy(
        piece_of(coarse_term, place, slot), coarse_terms_in.at[spot], local_sem.at[3]
    )
    term_self.start()

    arrive(1, fine_send, fine_block)
    part = compute(fine_block, fine_term)
    spread(3, fine_term, fine_own)
    fine_parts[group, me] = fine_term[me]
    tokens_grad[...] = (total[...] + part).astype(BF16)

    def hand_on(target, send_on, recv_on, p, step, landing_own):
        other = lax.rem(group + step, groups)
        landing = group if landing_own else other
        return pltpu.make_async_remote_copy(
            src_ref=target.at[group, p],
            dst_ref=target.at[landing, p],
            send_sem=send_on.at[other, p],
            recv_sem=recv_on.at[landing, p],
            device_id={"grp": other},
            device_id_type=MESH,
        )

    def relay(index, source, target, send_on, recv_on):
        own = target.at[group]

        def start(p):
            loop(1, groups, lambda step: hand_on(target, send_on, recv_on, p, step, True).start())

        def body(step):
            p = lax.rem(me + members - step, members)
            member_copy(index, source, own, p, False).wait_recv()
            start(p)

        start(me)
        loop(1, members, body)

    def relay_done(target, send_on, recv_on):
        def body(index):
            p = index // (groups - 1)
            step = lax.rem(index, groups - 1) + 1
            done = hand_on(target, send_on, recv_on, p, step, False)
            done.wait_recv()
            done.wait_send()

        if groups > 1:
            loop(0, members * (groups - 1), body)

    relay(2, middle_term, middle_parts, middle_send_on, middle_recv_on)

    loop(1, size, lambda step: team_copy(*gather_terms, step, False).wait_recv())
    term_self.wait()
    step_rows = min(rows, 16)
    weight = [
        [jnp.where(route(team_document(t), 0) == k, 1.0, 0.0) for k in range(coarse_count)]
        for t in range(size)
    ]

    def add_terms(index):
        z = index // (rows // step_rows)
        some = pl.ds(pl.multiple_of(lax.rem(index, rows // step_rows) * step_rows, step_rows), step_rows)
        pieces = [coarse_terms_in[t, z, some, :].astype(F32) for t in range(size)]
        for k in range(coarse_count):
            value = pieces[0] * weight[0][k]
            for t in range(1, size):
                value = value + pieces[t] * weight[t][k]
            coarse_sums[z, k, some, :] = value.astype(BF16)

    loop(0, outer * (rows // step_rows), add_terms)
    sum_stage = (1, lambda other: coarse_sums.at[other], coarse_sums_in)
    loop(1, outer, lambda step: line_copy(*sum_stage, step, True).start())
    coarse_sums_in[line] = coarse_sums[line]
    relay(3, fine_term, fine_parts, fine_send_on, fine_recv_on)


    left(0, middle_send, middle_block)
    left(1, fine_send, fine_block)
    group_left(*fine_trade)
    loop(1, outer, lambda step: line_copy(*first_stage, step, False).wait_send())
    loop(1, size, lambda step: team_copy(*second_stage, step, False).wait_send())
    loop(1, size, lambda step: team_copy(*gather_terms, step, False).wait_send())
    left(2, middle_term, middle_own)
    left(3, fine_term, fine_own)

    loop(1, outer, lambda step: line_copy(*sum_stage, step, False).wait_recv())
    value = coarse_sums_in[0].astype(F32)
    for z in range(1, outer):
        value = value + coarse_sums_in[z].astype(F32)
    coarse_total[...] = value.astype(BF16)
    coarse_trade = (1, lambda other: coarse_total, coarse_parts)
    group_spread(*coarse_trade)
    coarse_parts[group] = coarse_total[...]
    loop(1, outer, lambda step: line_copy(*sum_stage, step, False).wait_send())
    group_arrive(*coarse_trade)
    group_left(*coarse_trade)
    relay_done(middle_parts, middle_send_on, middle_recv_on)
    relay_done(fine_parts, fine_send_on, fine_recv_on)


def exchange(path, tokens, cotangent, coarse_w, middle_w, fine_w, groups, members):
    blocks, rows, wide = coarse_w.shape
    medium, narrow = middle_w.shape[2], fine_w.shape[2]
    token_count, width = tokens.shape
    count = groups * members
    outer, inner, team = plan(groups, members, wide)
    columns = wide // team
    size = team * inner

    def stack(*shape):
        return pltpu.VMEM(shape, BF16)

    def sems(*shape):
        return pltpu.SemaphoreType.DMA(shape)

    vmem = pl.BlockSpec(memory_space=pltpu.VMEM)
    return pl.pallas_call(
        functools.partial(main_kernel, groups, members),
        out_shape=(
            jax.ShapeDtypeStruct((count,) + path.shape, jnp.int32),
            jax.ShapeDtypeStruct(tokens.shape, BF16),
            jax.ShapeDtypeStruct((groups, members, rows, medium), BF16),
            jax.ShapeDtypeStruct((groups, members, rows, narrow), BF16),
            jax.ShapeDtypeStruct((groups, blocks, rows, columns), BF16),
        ),
        in_specs=[vmem] + [pl.BlockSpec(memory_space=pl.ANY)] * 5,
        out_specs=(vmem,) * 5,
        scratch_shapes=[
            pltpu.SMEM((count,) + path.shape, jnp.int32),
            stack(*tokens.shape),
            stack(*cotangent.shape),
            stack(*coarse_w.shape),
            stack(*middle_w.shape),
            stack(*fine_w.shape),
            stack(members, rows, medium),
            stack(groups, members, rows, narrow),
            stack(groups, members, rows, narrow),
            stack(members, rows, narrow),
            stack(outer, blocks, rows, columns),
            stack(size, outer, rows, columns),
            stack(outer, inner, rows, wide),
            stack(members, rows, medium),
            stack(members, rows, narrow),
            stack(outer, inner, rows, wide),
            stack(members, rows, medium),
            stack(members, rows, narrow),
            stack(size, outer, rows, columns),
            stack(outer, blocks, rows, columns),
            stack(outer, blocks, rows, columns),
            stack(blocks, rows, columns),
            stack(width, token_count),
            stack(width, token_count),
            pltpu.VMEM((token_count, width), F32),
            sems(count),
            sems(count),
            sems(4, members),
            sems(4, members),
            sems(2, groups),
            sems(2, groups),
            sems(2, outer),
            sems(2, outer),
            sems(2, size),
            sems(2, size),
            sems(4),
            sems(5),
            sems(groups, members),
            sems(groups, members),
            sems(groups, members),
            sems(groups, members),
        ],
        compiler_params=pltpu.CompilerParams(
            collective_id=0, has_side_effects=True, vmem_limit_bytes=60 * 2**20
        ),
        name="exchange",
    )(path, tokens, cotangent, coarse_w, middle_w, fine_w)


def collect_kernel(
    path,
    first_owned,
    tokens_in,
    middle_hbm,
    fine_hbm,
    coarse_parts,
    tokens_grad,
    coarse_grad,
    middle_grad,
    fine_grad,
    middle_parts,
    fine_parts,
    middle_sum,
    fine_sum,
    middle_last,
    fine_last,
    load_sem,
):
    count = middle_parts.shape[0]
    owned = fine_grad.shape[0]
    loads = (
        pltpu.make_async_copy(middle_hbm, middle_parts, load_sem.at[0]),
        pltpu.make_async_copy(fine_hbm, fine_parts, load_sem.at[1]),
    )
    for load in loads:
        load.start()
    middle_grad[...] = jnp.zeros_like(middle_grad)
    fine_grad[...] = jnp.zeros_like(fine_grad)
    middle_sum[count] = jnp.zeros(middle_sum.shape[1:], F32)
    fine_sum[count] = jnp.zeros(fine_sum.shape[1:], F32)
    for last in (middle_last, fine_last):

        def clear(k, carry, last=last):
            last[k] = count
            return carry

        lax.fori_loop(0, last.shape[0], clear, 0)
    tokens_grad[...] = tokens_in[...]
    groups, _, _, columns = coarse_parts.shape
    team = coarse_grad.shape[2] // columns
    for s in range(team):
        value = coarse_parts[s].astype(F32)
        for other in range(s + team, groups, team):
            value = value + coarse_parts[other].astype(F32)
        coarse_grad[:, :, s * columns : (s + 1) * columns] = value.astype(BF16)
    for load in loads:
        load.wait()

    def add(document, carry):
        k = path[document, 0, 1]
        value = middle_parts[document].astype(F32) + middle_sum[middle_last[k]]
        middle_sum[document] = value
        middle_grad[k] = value.astype(BF16)
        middle_last[k] = document
        place = path[document, 0, 2] - first_owned[0]

        @pl.when((place >= 0) & (place < owned))
        def _():
            piece = fine_parts[document].astype(F32) + fine_sum[fine_last[place]]
            fine_sum[document] = piece
            fine_grad[place] = piece.astype(BF16)
            fine_last[place] = document

        return carry

    lax.fori_loop(0, count, add, 0)


def collect(paths, first_owned, tokens_grad, middle_parts, fine_parts, coarse_parts, shapes):
    vmem = pl.BlockSpec(memory_space=pltpu.VMEM)
    smem = pl.BlockSpec(memory_space=pltpu.SMEM)
    hbm = pl.BlockSpec(memory_space=pl.ANY)
    count, rows, medium = middle_parts.shape
    narrow = fine_parts.shape[2]
    return pl.pallas_call(
        collect_kernel,
        out_shape=tuple(
            jax.ShapeDtypeStruct(shape, BF16) for shape in (tokens_grad.shape,) + shapes
        ),
        in_specs=[smem, smem, vmem, hbm, hbm, vmem],
        out_specs=(vmem,) * 4,
        scratch_shapes=[
            pltpu.VMEM(middle_parts.shape, BF16),
            pltpu.VMEM(fine_parts.shape, BF16),
            pltpu.VMEM((count + 1, rows, medium), F32),
            pltpu.VMEM((count + 1, rows, narrow), F32),
            pltpu.SMEM((shapes[1][0],), jnp.int32),
            pltpu.SMEM((shapes[2][0],), jnp.int32),
            pltpu.SemaphoreType.DMA((2,)),
        ],
        compiler_params=pltpu.CompilerParams(vmem_limit_bytes=60 * 2**20),
        name="collect",
    )(paths, first_owned, tokens_grad, middle_parts, fine_parts, coarse_parts)


def on_device(tokens, cotangent, path, coarse_weights, middle_weights, fine_weights):
    members = lax.axis_size("mem")
    groups = lax.axis_size("grp")
    paths, tokens_grad, middle_parts, fine_parts, coarse_parts = exchange(
        path, tokens, cotangent, coarse_weights, middle_weights, fine_weights, groups, members
    )
    first_owned = (lax.axis_index("grp") * fine_weights.shape[0]).astype(jnp.int32).reshape(1)
    flat = lambda parts: parts.reshape((groups * members,) + parts.shape[2:])
    return collect(
        paths,
        first_owned,
        tokens_grad,
        flat(middle_parts),
        flat(fine_parts),
        coarse_parts,
        (coarse_weights.shape, middle_weights.shape, fine_weights.shape),
    )


def solution(mesh):
    return jax.shard_map(
        on_device,
        mesh=mesh,
        in_specs=(
            P(("grp", "mem"), None),
            P(("grp", "mem"), None),
            P(("grp", "mem"), None),
            P(None, "mem", None),
            P(None, "mem", None),
            P("grp", "mem", None),
        ),
        out_specs=(
            P(("grp", "mem"), None),
            P(None, "mem", None),
            P(None, "mem", None),
            P("grp", "mem", None),
        ),
        check_vma=False,
    )
```
